256 devices in a mesh: outer: 4 (over y_hi, core), inner: 64 (over y_lo, z, x).
Axes of the slice: x: 4, y: 4 (y_hi: 2, y_lo: 2; y = y_hi * 2 + y_lo), z: 8, core: 2. Of those that a mesh axis runs over, the one named last changes fastest.
Arguments:
- queries: bfloat16 [32768, 2048], P(('outer', 'inner')), may hold values from -2 to 2
- keys: bfloat16 [32768, 2048], P(('outer', 'inner')), may hold values from -2 to 2
- values: bfloat16 [32768, 2048], P(('outer', 'inner')), may hold values from -6 to 6
- grad_out: bfloat16 [32768, 2048], P(('outer', 'inner')), may hold values from -96 to 96
- window: int32 [1], replicated, may hold values from 513 to 640
Outputs:
- query_grad: bfloat16 [32768, 2048], P(('outer', 'inner'))
- key_grad: bfloat16 [32768, 2048], P(('outer', 'inner'))
- value_grad: bfloat16 [32768, 2048], P(('outer', 'inner'))
The draws below stay inside these ranges and needn't reach their ends.
All inputs are finite; a program needn't handle non-finite values.
Results may differ from the reference program's by a relative error of at most 0.0085.
Values may be sent and summed in bfloat16 or wider, within the bound.
No kernel may reach another device: no remote copies, remote signals or barrier semaphores. Data moves between devices by JAX's collectives and lax.ppermute only.
A program may use at most 64 MiB of HBM per device.

```python
import jax
import jax.numpy as jnp
from jax import lax

TOK_DEV = 128
HEADS = 16
HD = 128
TOKENS = 32768


def shard_levels(own_key, shape, cuts, smallest, largest):
    loudness = 1.0
    for axis_at, blocks in cuts:
        heights = jax.random.uniform(jax.random.fold_in(jax.random.fold_in(own_key, 6), axis_at), (blocks,), jnp.float32, smallest / len(cuts), largest / len(cuts))
        loudness = loudness * jnp.repeat(jnp.exp(heights), shape[axis_at] // blocks).reshape((-1,) + (1,) * (len(shape) - 1 - axis_at))
    return loudness


def centred(stream_key, dims, scale, bound, cuts=(), kind=jnp.bfloat16):
    factor_of = shard_levels(stream_key, dims, cuts, -0.22, 0.18) if cuts else 1.0
    array = jax.random.normal(stream_key, dims, jnp.float32) * scale * factor_of
    return jnp.minimum(jnp.maximum(array, -bound), bound).astype(kind)


def setup_inputs(seed: int = 0) -> dict:
    splits = jax.random.split(jax.random.key(seed), 6)
    return {
        "queries": jnp.clip(jax.random.uniform(splits[0], (TOKENS, HEADS * HD), jnp.float32, -2.0, 2.0) * shard_levels(splits[0], (TOKENS, HEADS * HD), ((0, 256),), -0.4, 0.0), -2.0, 2.0).astype(jnp.bfloat16),
        "keys": jnp.clip(jax.random.uniform(splits[1], (TOKENS, HEADS * HD), jnp.float32, -2.0, 2.0) * shard_levels(splits[1], (TOKENS, HEADS * HD), ((0, 256),), -0.4, 0.0), -2.0, 2.0).astype(jnp.bfloat16),
        "values": centred(splits[2], (TOKENS, HEADS * HD), 1.0, 6.0, ((0, 256),)),
        "grad_out": centred(splits[3], (TOKENS, HEADS * HD), 16.0, 96.0, ((0, 256),)),
        "window": jax.random.randint(splits[4], (1,), 4 * TOK_DEV + 1, 5 * TOK_DEV + 1).astype(jnp.int32),
    }


def reference(queries, keys, values, grad_out, window):
    count = TOK_DEV
    shards = TOKENS // count
    scale = HD ** -0.5
    width = window[0]
    query_all = queries.reshape(TOKENS, HEADS, HD)
    grad_all = grad_out.reshape(TOKENS, HEADS, HD)
    filler = jnp.zeros((5 * count, HEADS * HD), keys.dtype)
    key_pad = jnp.concatenate([filler, keys], axis=0).reshape(-1, HEADS, HD)
    value_pad = jnp.concatenate([filler, values], axis=0).reshape(-1, HEADS, HD)

    def step(carry, index):
        key_acc, value_acc = carry
        begin = (index * count).astype(jnp.int32)
        query_block = lax.dynamic_slice_in_dim(query_all, begin, count, 0).astype(jnp.float32)
        grad_block = lax.dynamic_slice_in_dim(grad_all, begin, count, 0).astype(jnp.float32)
        key_block = lax.dynamic_slice_in_dim(key_pad, begin, 6 * count, 0).astype(jnp.float32)
        value_block = lax.dynamic_slice_in_dim(value_pad, begin, 6 * count, 0).astype(jnp.float32)
        query_pos = begin + jnp.arange(count, dtype=jnp.int32)[:, None]
        key_pos = begin - 5 * count + jnp.arange(6 * count, dtype=jnp.int32)[None, :]
        allowed = (key_pos <= query_pos) & (key_pos > query_pos - width) & (key_pos >= 0)
        logits = jnp.einsum("qhd,khd->hqk", query_block, key_block) * scale
        weights = jnp.where(allowed[None], jnp.exp(logits), jnp.float32(0.0))
        norm_total = jnp.sum(weights, axis=2)
        weights_low = lax.optimization_barrier(weights.astype(jnp.bfloat16)).astype(jnp.float32)
        weighted = jnp.einsum("hqk,khd->qhd", weights_low, value_block)
        output = weighted / jnp.transpose(norm_total)[:, :, None]
        centre = jnp.transpose(jnp.sum(grad_block * output, axis=2))
        log_norm = jnp.log(norm_total)
        probs = jnp.where(allowed[None], jnp.exp(logits - log_norm[:, :, None]), jnp.float32(0.0))
        probs_low = lax.optimization_barrier(probs.astype(jnp.bfloat16)).astype(jnp.float32)
        prob_grad = jnp.einsum("qhd,khd->hqk", grad_block, value_block)
        logit_grad = probs * (prob_grad - centre[:, :, None])
        logit_low = lax.optimization_barrier(logit_grad.astype(jnp.bfloat16)).astype(jnp.float32)
        logit_split = logit_low.reshape(HEADS, count, 6, count)
        probs_split = probs_low.reshape(HEADS, count, 6, count)
        key_split = key_block.reshape(6, count, HEADS, HD)
        query_terms = (jnp.einsum("hqec,echd->eqhd", logit_split, key_split) * scale).astype(jnp.bfloat16)
        query_sum = jnp.sum(query_terms.astype(jnp.float32), axis=0)
        key_terms = (jnp.einsum("hqec,qhd->echd", logit_split, query_block) * scale).astype(jnp.bfloat16)
        value_terms = jnp.einsum("hqec,qhd->echd", probs_split, grad_block).astype(jnp.bfloat16)
        key_terms = key_terms.astype(jnp.float32).reshape(6 * count, HEADS, HD)
        value_terms = value_terms.astype(jnp.float32).reshape(6 * count, HEADS, HD)
        key_acc = lax.dynamic_update_slice_in_dim(key_acc, lax.dynamic_slice_in_dim(key_acc, begin, 6 * count, 0) + key_terms, begin, 0)
        value_acc = lax.dynamic_update_slice_in_dim(value_acc, lax.dynamic_slice_in_dim(value_acc, begin, 6 * count, 0) + value_terms, begin, 0)
        return (key_acc, value_acc), query_sum.astype(jnp.bfloat16)

    start_acc = jnp.zeros(((shards + 5) * count, HEADS, HD), jnp.float32)
    carry, query_parts = lax.scan(step, (start_acc, start_acc), jnp.arange(shards, dtype=jnp.int32))
    key_acc, value_acc = carry
    query_grad = query_parts.reshape(TOKENS, HEADS * HD)
    key_grad = key_acc[5 * count:].reshape(TOKENS, HEADS * HD).astype(jnp.bfloat16)
    value_grad = value_acc[5 * count:].reshape(TOKENS, HEADS * HD).astype(jnp.bfloat16)
    return (query_grad, key_grad, value_grad)
```

```python
import functools
import math

import jax
import jax.numpy as jnp
import numpy as np
from jax import lax
from jax.experimental import pallas as pl
from jax.experimental.pallas import tpu as pltpu
from jax.sharding import Mesh
from jax.sharding import PartitionSpec as P

HEADS = 16
HD = 128
BLK = 128
SIDE = 4
HH = HEADS // SIDE
SCALE = HD ** (-0.5)
SCALE2 = SCALE * math.log2(math.e)
OFF = -1e30
SEQ = ("o", "yl", "z")

NT = (((1,), (1,)), ((), ()))
NN = (((1,), (0,)), ((), ()))


def dot(a, b, dims):
    return lax.dot_general(a, b, dims, preferred_element_type=jnp.float32)


def tiles(width, axis):
    key = lax.broadcasted_iota(jnp.int32, (BLK, BLK), axis)
    query = lax.broadcasted_iota(jnp.int32, (BLK, BLK), 1 - axis)
    back = query - key
    zero = jnp.zeros((BLK, BLK), jnp.float32)
    return {
        0: jnp.where(back >= 0, zero, OFF),
        4: jnp.where(back + 4 * BLK < width, zero, OFF),
        5: jnp.where(back + 5 * BLK < width, zero, OFF),
    }


def query_kernel(scal, qg, kv, kvp, kvpp, dq, stats, cols, bias):
    width, has1, has2 = scal[0], scal[1], scal[2]
    for at, (_, tile) in enumerate(sorted(tiles(width, 1).items())):
        bias[at] = tile
    cols[...] = jnp.zeros_like(cols)
    lane = lax.broadcasted_iota(jnp.int32, (BLK, BLK), 1)
    off1 = jnp.where(has1 > 0, 0.0, OFF).astype(jnp.float32)
    off2 = jnp.where(has2 > 0, 0.0, OFF).astype(jnp.float32)

    def block(at, which, h):
        if at == 0:
            return kvpp[which, h]
        if at < 5:
            return kvp[at - 1, which, h]
        return kv[at - 5, which, h]

    def head(h, carry):
        for j in range(4):
            query = qg[j, 0, h]
            grad = qg[j, 1, h]
            weights, products = [], []
            norm = jnp.zeros((BLK, 1), jnp.float32)
            centre = jnp.zeros((BLK, 1), jnp.float32)
            for hop in range(6):
                at = j + 5 - hop
                logits = dot(query, block(at, 0, h), NT) * SCALE2
                if hop in (0, 4, 5):
                    logits = logits + bias[{0: 0, 4: 1, 5: 2}[hop]]
                if at < 5:
                    logits = logits + (off2 if at == 0 else off1)
                weight = jnp.exp2(logits)
                product = dot(grad, block(at, 1, h), NT)
                norm = norm + jnp.sum(weight, axis=1, keepdims=True)
                centre = centre + jnp.sum(weight * product, axis=1, keepdims=True)
                weights.append(weight)
                products.append(product)
            inverse = 1.0 / norm
            centre = centre * inverse
            total = jnp.zeros((BLK, HD), jnp.float32)
            for hop in range(6):
                at = j + 5 - hop
                change = (weights[hop] * inverse) * (products[hop] - centre)
                total = total + dot(change.astype(jnp.bfloat16), block(at, 0, h), NN)
            dq[j, h] = (total * SCALE).astype(jnp.bfloat16)
            row = j * 8 + h
            cols[...] = jnp.where(
                lane == row, jnp.log2(norm), jnp.where(lane == row + 4, centre, cols[...])
            )
        return carry

    lax.fori_loop(0, HH, head, 0)
    stats[...] = jnp.transpose(cols[...])[:32]


def key_pairs(j, h, hops, key, value, queries, stats_of, bias, dk, dv):
    for hop in hops:
        query, grad = queries(j + hop, h)
        log_norm, centre = stats_of(j + hop, h)
        logits = dot(key, query, NT) * SCALE2 - log_norm
        if hop in (0, 4, 5):
            logits = logits + bias[{0: 0, 4: 1, 5: 2}[hop]]
        probs = jnp.exp2(logits)
        product = dot(value, grad, NT)
        dv = dv + dot(probs.astype(jnp.bfloat16), grad, NN)
        change = probs * (product - centre)
        dk = dk + dot(change.astype(jnp.bfloat16), query, NN)
    return dk, dv


def own_key_kernel(scal, qg, kv, stats, part, bias):
    for at, (_, tile) in enumerate(sorted(tiles(scal[0], 0).items())):
        bias[at] = tile

    def stats_of(at, h):
        return stats[pl.ds(at * 8 + h, 1)], stats[pl.ds(at * 8 + 4 + h, 1)]

    def head(h, carry):
        for j in range(4):
            zero = jnp.zeros((BLK, HD), jnp.float32)
            dk, dv = key_pairs(
                j, h, range(0, 4 - j), kv[j, 0, h], kv[j, 1, h],
                lambda at, h: (qg[at, 0, h], qg[at, 1, h]), stats_of, bias, zero, zero,
            )
            part[j, 0, h] = dk
            part[j, 1, h] = dv
        return carry

    lax.fori_loop(0, HH, head, 0)


def far_key_kernel(scal, qgn, qgnn, kv, stats, far_stats, part, out, bias):
    for at, (_, tile) in enumerate(sorted(tiles(scal[0], 0).items())):
        bias[at] = tile

    def queries(at, h):
        if at == 8:
            return qgnn[0, h], qgnn[1, h]
        return qgn[at - 4, 0, h], qgn[at - 4, 1, h]

    def stats_of(at, h):
        if at == 8:
            return far_stats[pl.ds(h, 1)], far_stats[pl.ds(4 + h, 1)]
        row = (at - 4) * 8 + h
        return stats[pl.ds(row, 1)], stats[pl.ds(row + 4, 1)]

    def head(h, carry):
        for j in range(4):
            dk, dv = key_pairs(
                j, h, range(4 - j, 6), kv[j, 0, h], kv[j, 1, h],
                queries, stats_of, bias, part[j, 0, h], part[j, 1, h],
            )
            out[j, 0, h] = (dk * SCALE).astype(jnp.bfloat16)
            out[j, 1, h] = dv.astype(jnp.bfloat16)
        return carry

    lax.fori_loop(0, HH, head, 0)


def call(kernel, outs, scratch, *args):
    specs = [pl.BlockSpec(memory_space=pltpu.SMEM)]
    specs += [pl.BlockSpec(memory_space=pltpu.VMEM) for _ in args[1:]]
    return pl.pallas_call(
        kernel,
        out_shape=outs,
        in_specs=specs,
        out_specs=jax.tree.map(lambda _: pl.BlockSpec(memory_space=pltpu.VMEM), outs),
        scratch_shapes=scratch,
        compiler_params=pltpu.CompilerParams(vmem_limit_bytes=40 * 1024 * 1024),
    )(*args)


def shift(value, steps):
    count = lax.axis_size(SEQ)
    pairs = [(at, at + steps) for at in range(count) if 0 <= at + steps < count]
    return lax.ppermute(value, SEQ, pairs)


def spread(first, second):
    both = jnp.stack([first, second]).reshape(2, BLK, SIDE, HH, HD)
    return lax.all_to_all(jnp.transpose(both, (2, 0, 3, 1, 4)), "x", 0, 0)


def gather_back(blocks):
    mine = lax.all_to_all(blocks, "x", 0, 0)
    return mine


def flat(mine):
    return jnp.transpose(mine, (2, 0, 1, 3)).reshape(BLK, HEADS * HD)


def per_device(queries, keys, values, grad_out, window):
    f32 = jnp.float32
    group = lax.axis_index(SEQ)
    scal = jnp.stack(
        [window[0], (group >= 1).astype(jnp.int32), (group >= 2).astype(jnp.int32)]
    ).astype(jnp.int32)
    kv = spread(keys, values)
    last = shift(kv[3], 1)
    rest = shift(kv[:3], 1)
    kvpp = shift(last, 1)
    kvp = jnp.concatenate([rest, last[None]])
    qg = spread(queries, grad_out)
    head0 = shift(qg[0], -1)
    rest_q = shift(qg[1:], -1)
    qgnn = shift(head0, -1)
    qgn = jnp.concatenate([head0[None], rest_q])
    tile = (3, BLK, BLK)
    dq, stats = call(
        query_kernel,
        [
            jax.ShapeDtypeStruct((SIDE, HH, BLK, HD), jnp.bfloat16),
            jax.ShapeDtypeStruct((32, BLK), f32),
        ],
        [pltpu.VMEM((BLK, BLK), f32), pltpu.VMEM(tile, f32)],
        scal, qg, kv, kvp, kvpp,
    )
    near_stats = shift(stats, -1)
    far_stats = shift(stats[:8], -2)
    query_grad = flat(gather_back(dq))
    part = call(
        own_key_kernel,
        jax.ShapeDtypeStruct((SIDE, 2, HH, BLK, HD), f32),
        [pltpu.VMEM(tile, f32)],
        scal, qg, kv, stats,
    )
    dkv = call(
        far_key_kernel,
        jax.ShapeDtypeStruct((SIDE, 2, HH, BLK, HD), jnp.bfloat16),
        [pltpu.VMEM(tile, f32)],
        scal, qgn, qgnn, kv, near_stats, far_stats, part,
    )
    back = gather_back(dkv)
    return query_grad, flat(back[:, 0]), flat(back[:, 1])


def solution(mesh):
    cube = Mesh(np.asarray(mesh.devices).reshape(4, 2, 8, SIDE), SEQ + ("x",))
    rows = P(SEQ + ("x",), None)
    return jax.shard_map(
        per_device,
        mesh=cube,
        in_specs=(rows, rows, rows, rows, P()),
        out_specs=(rows, rows, rows),
        check_vma=False,
    )
```

```python
import math

import jax
import jax.numpy as jnp
import numpy as np
from jax import lax
from jax.experimental import pallas as pl
from jax.experimental.pallas import tpu as pltpu
from jax.sharding import Mesh
from jax.sharding import PartitionSpec as P


HEADS = 16
HD = 128
BLK = 128
SIDE = 4
HC = HEADS // SIDE
SCALE = HD ** (-0.5)
SCALE2 = SCALE * math.log2(math.e)
OFF = -1e30
GROUPS = ("o", "yl", "z")
INSIDE = "x"
BF = jnp.bfloat16
F32 = jnp.float32

NT = (((1,), (1,)), ((), ()))
NN = (((1,), (0,)), ((), ()))


def dot(a, b, dims):
    return lax.dot_general(a, b, dims, preferred_element_type=F32)


def mask_tile(width, blocks, shape, query_axis):
    query = lax.broadcasted_iota(jnp.int32, shape, query_axis)
    key = lax.broadcasted_iota(jnp.int32, shape, 1 - query_axis)
    back = query - key + blocks * BLK
    return jnp.where((back >= 0) & (back < width), 0.0, OFF).astype(F32)


def pack_kernel(first, second, out, sems):
    copies = []
    for dest in range(SIDE):
        for which, ref in enumerate((first, second)):
            for h in range(HC):
                lane = (dest * HC + h) * HD
                copies.append(
                    pltpu.make_async_copy(
                        ref.at[:, lane : lane + HD], out.at[dest, which, h], sems.at[len(copies)]
                    )
                )
    for copy in copies:
        copy.start()
    for copy in copies:
        copy.wait()


def unpack_kernel(back, *rest):
    outs, sems = rest[:-1], rest[-1]
    copies = []
    for which, out in enumerate(outs):
        for source in range(SIDE):
            for h in range(HC):
                lane = (source * HC + h) * HD
                copies.append(
                    pltpu.make_async_copy(
                        back.at[source, which, h], out.at[:, lane : lane + HD], sems.at[len(copies)]
                    )
                )
    for copy in copies:
        copy.start()
    for copy in copies:
        copy.wait()


def joined(blocks):
    return blocks[0] if len(blocks) == 1 else jnp.concatenate(blocks, axis=0)


A_TILES = (5, 4, 3, 0, -1)
A_STEPS = ((0, 1), (2, 3), (4, 5), (6,))


def fill_a(width, bias):
    for at, blocks in enumerate(A_TILES):
        bias[at] = mask_tile(width, blocks, (2 * BLK, BLK), 0)


def query_half(j, h, group, qg, keys, bias, wts, prods, cols):
    shape = (2 * BLK, BLK)
    query = joined([qg[j, 0, h], qg[j + 1, 0, h]])
    grad = joined([qg[j, 1, h], qg[j + 1, 1, h]])
    norm = jnp.zeros(shape, F32)
    centre = jnp.zeros(shape, F32)
    for steps in A_STEPS:
        logits2 = dot(query, joined([keys(j + s, 0, h) for s in steps]), NT)
        product2 = dot(grad, joined([keys(j + s, 1, h) for s in steps]), NT)
        for part, step in enumerate(steps):
            at, blocks = j + step, 5 - step
            logits = logits2[:, part * BLK : (part + 1) * BLK] * SCALE2
            product = product2[:, part * BLK : (part + 1) * BLK]
            if blocks in A_TILES:
                logits = logits + bias[A_TILES.index(blocks)]
            if at <= SIDE:
                behind = group > 0 if at else group > 1
                logits = logits + jnp.where(behind, 0.0, OFF).astype(F32)
            weight = jnp.exp2(logits)
            wts[step] = weight
            prods[step] = product
            norm = norm + weight
            centre = centre + weight * product
    norm = jnp.sum(norm, axis=1, keepdims=True)
    inverse = 1.0 / norm
    centre = jnp.sum(centre, axis=1, keepdims=True) * inverse
    total = jnp.zeros(shape, F32)
    for steps in A_STEPS:
        change = [(wts[s] * inverse) * (prods[s] - centre) for s in steps]
        change = change[0] if len(steps) == 1 else jnp.concatenate(change, axis=1)
        total = total + dot(change.astype(BF), joined([keys(j + s, 0, h) for s in steps]), NN)
    lane = lax.broadcasted_iota(jnp.int32, shape, 1)
    cols[...] = jnp.where(
        lane == h, jnp.log2(norm), jnp.where(lane == HC + h, centre, cols[...])
    )
    return (total * SCALE).astype(BF)


def rows_of(cols):
    rows = jnp.transpose(cols[...])[:8]
    return rows[:, :BLK], rows[:, BLK:]


def early_kernel(scal, qg, kv, kvp, dq, stats, part, cols, bias, bias_b, wts, prods):
    fill_a(scal[0], bias)
    fill_b(scal[0], bias_b)
    cols[...] = jnp.zeros_like(cols)

    def keys(at, which, h):
        return kvp[at - 1, which, h] if at <= SIDE else kv[at - SIDE - 1, which, h]

    def head(h, carry):
        total = query_half(2, h, scal[1], qg, keys, bias, wts, prods, cols)
        dq[0, 0, h] = total[:BLK]
        dq[1, 0, h] = total[BLK:]
        return carry

    lax.fori_loop(0, HC, head, 0)
    stats[:8], stats[8:] = rows_of(cols)

    def key_head(h, carry):
        for half, steps in ((0, (2, 3)), (1, (0, 1))):
            j = 2 * half
            zero = jnp.zeros((2 * BLK, HD), F32)
            dk, dv = key_half(
                [steps],
                joined([kv[j, 0, h], kv[j + 1, 0, h]]),
                joined([kv[j, 1, h], kv[j + 1, 1, h]]),
                lambda s, which: qg[j + s, which, h],
                lambda s: stats_rows(stats, j + s - 2, h),
                bias_b, zero, zero,
            )
            part[half, 0, h] = dk
            part[half, 1, h] = dv
        return carry

    lax.fori_loop(0, HC, key_head, 0)


def query_kernel(scal, qg, kv, kvp, kvpp, dq_late, stats_late, dq, stats, front, cols, bias, wts, prods):
    fill_a(scal[0], bias)
    cols[...] = jnp.zeros_like(cols)
    dq[2:] = dq_late[...]
    stats[16:] = stats_late[...]

    def keys(at, which, h):
        if at == 0:
            return kvpp[which, h]
        return kvp[at - 1, which, h] if at <= SIDE else kv[at - SIDE - 1, which, h]

    def head(h, carry):
        total = query_half(0, h, scal[1], qg, keys, bias, wts, prods, cols)
        dq[0, 0, h] = total[:BLK]
        dq[1, 0, h] = total[BLK:]
        return carry

    lax.fori_loop(0, HC, head, 0)
    first, second = rows_of(cols)
    front[...] = first
    stats[:8] = first
    stats[8:16] = second


def stats_rows(stats, block, h):
    return stats[pl.ds(block * 8 + h, 1)], stats[pl.ds(block * 8 + HC + h, 1)]


B_TILES = (0, 1, 4, 5, 6)


def fill_b(width, bias):
    for at, blocks in enumerate(B_TILES):
        bias[at] = mask_tile(width, blocks, (2 * BLK, BLK), 1)


def key_half(steps_of, key, value, queries, stats_of, bias, dk, dv):
    for steps in steps_of:
        query = joined([queries(s, 0) for s in steps])
        grad = joined([queries(s, 1) for s in steps])
        logits2 = dot(key, query, NT)
        product2 = dot(value, grad, NT)
        probs2, change2 = [], []
        for part, step in enumerate(steps):
            log_norm, centre = stats_of(step)
            logits = logits2[:, part * BLK : (part + 1) * BLK] * SCALE2 - log_norm
            if step in B_TILES:
                logits = logits + bias[B_TILES.index(step)]
            probs = jnp.exp2(logits)
            probs2.append(probs.astype(BF))
            change = probs * (product2[:, part * BLK : (part + 1) * BLK] - centre)
            change2.append(change.astype(BF))
        probs2 = probs2[0] if len(steps) == 1 else jnp.concatenate(probs2, axis=1)
        change2 = change2[0] if len(steps) == 1 else jnp.concatenate(change2, axis=1)
        dv = dv + dot(probs2, grad, NN)
        dk = dk + dot(change2, query, NN)
    return dk, dv


def far_key_kernel(
    scal, qg, qgn, qgnn, kv, stats, near, after, part_hbm, out, bias, part, sem
):
    fetch = pltpu.make_async_copy(part_hbm, part, sem)
    fetch.start()
    fill_b(scal[0], bias)

    def queries(at, which, h):
        if at < SIDE:
            return qg[at, which, h]
        return qgnn[which, h] if at == 2 * SIDE else qgn[at - SIDE, which, h]

    def stats_of(at, h):
        if at < SIDE:
            return stats_rows(stats, at, h)
        return stats_rows(after, 0, h) if at == 2 * SIDE else stats_rows(near, at - SIDE, h)

    fetch.wait()

    def head(h, carry):
        for half, todo in ((0, ((0, 1), (4, 5), (6,))), (1, ((2, 3), (4, 5), (6,)))):
            j = 2 * half
            dk, dv = key_half(
                todo,
                joined([kv[j, 0, h], kv[j + 1, 0, h]]),
                joined([kv[j, 1, h], kv[j + 1, 1, h]]),
                lambda s, which: queries(j + s, which, h),
                lambda s: stats_of(j + s, h),
                bias, part[half, 0, h], part[half, 1, h],
            )
            dk = (dk * SCALE).astype(BF)
            dv = dv.astype(BF)
            out[j, 0, h] = dk[:BLK]
            out[j + 1, 0, h] = dk[BLK:]
            out[j, 1, h] = dv[:BLK]
            out[j + 1, 1, h] = dv[BLK:]
        return carry

    lax.fori_loop(0, HC, head, 0)


VM = pl.BlockSpec(memory_space=pltpu.VMEM)
HBM = pl.BlockSpec(memory_space=pltpu.HBM)
PARAMS = pltpu.CompilerParams(vmem_limit_bytes=20 * 1024 * 1024)


def call(kernel, outs, scratch, scal, *args, specs=None):
    return pl.pallas_call(
        kernel,
        out_shape=outs,
        in_specs=[pl.BlockSpec(memory_space=pltpu.SMEM)] + (specs or [VM for _ in args]),
        out_specs=jax.tree.map(lambda _: VM, outs),
        scratch_shapes=scratch,
        compiler_params=PARAMS,
    )(scal, *args)


def in_hbm(value):
    return pltpu.with_memory_space_constraint(value, pltpu.HBM)


def blocks_of(arrays, blocks=SIDE):
    return jax.ShapeDtypeStruct((blocks, arrays, HC, BLK, HD), BF)


def pack(first, second):
    return pl.pallas_call(
        pack_kernel,
        out_shape=blocks_of(2),
        in_specs=[HBM, HBM],
        out_specs=VM,
        scratch_shapes=[pltpu.SemaphoreType.DMA((2 * HEADS,))],
        compiler_params=PARAMS,
    )(in_hbm(first), in_hbm(second))


def unpack(back):
    arrays = back.shape[1]
    rows = jax.ShapeDtypeStruct((BLK, HEADS * HD), BF)
    return pl.pallas_call(
        unpack_kernel,
        out_shape=[rows] * arrays,
        in_specs=[VM],
        out_specs=[HBM] * arrays,
        scratch_shapes=[pltpu.SemaphoreType.DMA((arrays * HEADS,))],
        compiler_params=PARAMS,
    )(back)


def shift(value, steps):
    count = lax.axis_size(GROUPS)
    pairs = [(at, at + steps) for at in range(count) if 0 <= at + steps < count]
    return lax.ppermute(value, GROUPS, pairs)


def swap(value):
    return lax.all_to_all(value, INSIDE, 0, 0)


def steps(queries, keys, values, grad_out, window):
    group = lax.axis_index(GROUPS)
    scal = jnp.stack([window[0], group]).astype(jnp.int32)
    packed = pack(keys, values)
    kv = swap(packed)
    packed = pack(queries, grad_out)
    raw = shift(packed, -1)
    kvp = shift(kv, 1)
    kvpp = shift(kv[SIDE - 1], 2)
    qg = swap(packed)
    qgnn = shift(qg[0], -2)
    qgn = swap(raw)
    tiles = pltpu.VMEM((5, 2 * BLK, BLK), F32)
    row_tiles = pltpu.VMEM((7, 2 * BLK, BLK), F32)
    cols = pltpu.VMEM((2 * BLK, BLK), F32)
    part_shape = (SIDE // 2, 2, HC, 2 * BLK, HD)
    dq_late, stats_late, part = call(
        early_kernel,
        [
            blocks_of(1, 2),
            jax.ShapeDtypeStruct((16, BLK), F32),
            jax.ShapeDtypeStruct(part_shape, F32),
        ],
        [cols, tiles, tiles, row_tiles, row_tiles],
        scal, qg, kv, kvp,
    )
    dq, stats, front = call(
        query_kernel,
        [
            blocks_of(1),
            jax.ShapeDtypeStruct((8 * SIDE, BLK), F32),
            jax.ShapeDtypeStruct((8, BLK), F32),
        ],
        [cols, tiles, row_tiles, row_tiles],
        scal, qg, kv, kvp, kvpp, dq_late, stats_late,
    )
    near = shift(stats, -1)
    after = shift(front, -2)
    back = swap(in_hbm(dq))
    (query_grad,) = unpack(back)
    dkv = call(
        far_key_kernel, blocks_of(2),
        [tiles, pltpu.VMEM(part_shape, F32), pltpu.SemaphoreType.DMA(())],
        scal, qg, qgn, qgnn, kv, stats, near, after, in_hbm(part),
        specs=[VM] * 7 + [HBM],
    )
    back = swap(dkv)
    key_grad, value_grad = unpack(back)
    return query_grad, key_grad, value_grad


def solution(mesh):
    cube = Mesh(np.asarray(mesh.devices).reshape(4, 2, 8, SIDE), GROUPS + ("x",))
    rows = P(GROUPS + ("x",), None)
    return jax.shard_map(
        steps,
        mesh=cube,
        in_specs=(rows, rows, rows, rows, P()),
        out_specs=(rows, rows, rows),
        check_vma=False,
    )
```

```python
import math

import jax
import jax.numpy as jnp
import numpy as np
from jax import lax
from jax.experimental import pallas as pl
from jax.experimental.pallas import tpu as pltpu
from jax.sharding import Mesh
from jax.sharding import PartitionSpec as P


HEADS = 16
HD = 128
BLK = 128
SIDE = 4
HC = HEADS // SIDE
SCALE = HD ** (-0.5)
SCALE2 = SCALE * math.log2(math.e)
OFF = -1e30
GROUPS = ("o", "yl", "z")
INSIDE = "x"
BF = jnp.bfloat16
F32 = jnp.float32

NT = (((1,), (1,)), ((), ()))
NN = (((1,), (0,)), ((), ()))


def dot(a, b, dims):
    return lax.dot_general(a, b, dims, preferred_element_type=F32)


def mask_tile(width, blocks, shape, query_axis):
    query = lax.broadcasted_iota(jnp.int32, shape, query_axis)
    key = lax.broadcasted_iota(jnp.int32, shape, 1 - query_axis)
    back = query - key + blocks * BLK
    return jnp.where((back >= 0) & (back < width), 0.0, OFF).astype(F32)


def pack_kernel(first, second, out, sems):
    copies = []
    for dest in range(SIDE):
        for which, ref in enumerate((first, second)):
            for h in range(HC):
                lane = (dest * HC + h) * HD
                copies.append(
                    pltpu.make_async_copy(
                        ref.at[:, lane : lane + HD], out.at[dest, which, h], sems.at[len(copies)]
                    )
                )
    for copy in copies:
        copy.start()
    for copy in copies:
        copy.wait()


def unpack_kernel(back, *rest):
    outs, sems = rest[:-1], rest[-1]
    copies = []
    for which, out in enumerate(outs):
        for source in range(SIDE):
            for h in range(HC):
                lane = (source * HC + h) * HD
                copies.append(
                    pltpu.make_async_copy(
                        back.at[source, which, h], out.at[:, lane : lane + HD], sems.at[len(copies)]
                    )
                )
    for copy in copies:
        copy.start()
    for copy in copies:
        copy.wait()


def joined(blocks):
    return blocks[0] if len(blocks) == 1 else jnp.concatenate(blocks, axis=0)


A_TILES = (5, 4, 3, 0, -1)
A_STEPS = ((0, 1), (2, 3), (4, 5), (6,))


def fill_a(width, bias):
    for at, blocks in enumerate(A_TILES):
        bias[at] = mask_tile(width, blocks, (2 * BLK, BLK), 0)


def query_half(j, h, group, qg, keys, bias, wts, prods, cols):
    shape = (2 * BLK, BLK)
    query = joined([qg[j, 0, h], qg[j + 1, 0, h]])
    grad = joined([qg[j, 1, h], qg[j + 1, 1, h]])
    norm = jnp.zeros(shape, F32)
    centre = jnp.zeros(shape, F32)
    for steps in A_STEPS:
        logits2 = dot(query, joined([keys(j + s, 0, h) for s in steps]), NT)
        product2 = dot(grad, joined([keys(j + s, 1, h) for s in steps]), NT)
        for part, step in enumerate(steps):
            at, blocks = j + step, 5 - step
            logits = logits2[:, part * BLK : (part + 1) * BLK] * SCALE2
            product = product2[:, part * BLK : (part + 1) * BLK]
            if blocks in A_TILES:
                logits = logits + bias[A_TILES.index(blocks)]
            if at <= SIDE:
                behind = group > 0 if at else group > 1
                logits = logits + jnp.where(behind, 0.0, OFF).astype(F32)
            weight = jnp.exp2(logits)
            wts[h % 2, step] = weight
            prods[h % 2, step] = product
            norm = norm + weight
            centre = centre + weight * product
    norm = jnp.sum(norm, axis=1, keepdims=True)
    inverse = 1.0 / norm
    centre = jnp.sum(centre, axis=1, keepdims=True) * inverse
    total = jnp.zeros(shape, F32)
    for steps in A_STEPS:
        change = [(wts[h % 2, s] * inverse) * (prods[h % 2, s] - centre) for s in steps]
        change = change[0] if len(steps) == 1 else jnp.concatenate(change, axis=1)
        total = total + dot(change.astype(BF), joined([keys(j + s, 0, h) for s in steps]), NN)
    lane = lax.broadcasted_iota(jnp.int32, shape, 1)
    cols[...] = jnp.where(
        lane == h, jnp.log2(norm), jnp.where(lane == HC + h, centre, cols[...])
    )
    return (total * SCALE).astype(BF)


def rows_of(cols):
    rows = jnp.transpose(cols[...])[:8]
    return rows[:, :BLK], rows[:, BLK:]


def head_copy(source, target, sems, h):
    return pltpu.make_async_copy(source.at[:, :, h], target.at[:, :, h], sems.at[h])


def finish_heads(source, target, sems):
    for h in range(HC):
        head_copy(source, target, sems, h).wait()


def fetch_heads(source, target, sems):
    def copy(h):
        return head_copy(source, target, sems, h)

    for h in range(HC):
        copy(h).start()
    return lambda h: copy(h).wait()


def early_kernel(
    scal, qg, kv, kvp_hbm, dq, stats, part_hbm, cols, bias, bias_b, wts, prods, kvp, part, sems, sems_out
):
    arrived = fetch_heads(kvp_hbm, kvp, sems)
    fill_a(scal[0], bias)
    fill_b(scal[0], bias_b)
    cols[...] = jnp.zeros_like(cols)

    def keys(at, which, h):
        return kvp[at - 1, which, h] if at <= SIDE else kv[at - SIDE - 1, which, h]

    def head(h):
        arrived(h)
        total = query_half(2, h, scal[1], qg, keys, bias, wts, prods, cols)
        dq[0, 0, h] = total[:BLK]
        dq[1, 0, h] = total[BLK:]

    for h in range(HC):
        head(h)
    stats[:8], stats[8:] = rows_of(cols)

    def key_head(h):
        for half, steps in ((0, (2, 3)), (1, (0, 1))):
            j = 2 * half
            zero = jnp.zeros((2 * BLK, HD), F32)
            dk, dv = key_half(
                [steps],
                joined([kv[j, 0, h], kv[j + 1, 0, h]]),
                joined([kv[j, 1, h], kv[j + 1, 1, h]]),
                lambda s, which: qg[j + s, which, h],
                lambda s: stats_rows(stats, j + s - 2, h),
                bias_b, zero, zero,
            )
            part[half, 0, h] = dk
            part[half, 1, h] = dv
        head_copy(part, part_hbm, sems_out, h).start()

    for h in range(HC):
        key_head(h)
    finish_heads(part, part_hbm, sems_out)


def query_kernel(
    scal, qg, kv, kvp_hbm, kvpp, dq_late, stats_late, dq_hbm, stats, front,
    cols, bias, wts, prods, kvp, dq_own, sems, sems_out,
):
    arrived = fetch_heads(kvp_hbm, kvp, sems)
    fill_a(scal[0], bias)
    cols[...] = jnp.zeros_like(cols)
    dq_own[2:] = dq_late[...]
    stats[16:] = stats_late[...]

    def keys(at, which, h):
        if at == 0:
            return kvpp[which, h]
        return kvp[at - 1, which, h] if at <= SIDE else kv[at - SIDE - 1, which, h]

    def head(h):
        arrived(h)
        total = query_half(0, h, scal[1], qg, keys, bias, wts, prods, cols)
        dq_own[0, 0, h] = total[:BLK]
        dq_own[1, 0, h] = total[BLK:]
        head_copy(dq_own, dq_hbm, sems_out, h).start()

    for h in range(HC):
        head(h)
    first, second = rows_of(cols)
    front[...] = first
    stats[:8] = first
    stats[8:16] = second
    finish_heads(dq_own, dq_hbm, sems_out)


def stats_rows(stats, block, h):
    return stats[block * 8 + h : block * 8 + h + 1], stats[block * 8 + HC + h : block * 8 + HC + h + 1]


B_TILES = (0, 1, 4, 5, 6)


def fill_b(width, bias):
    for at, blocks in enumerate(B_TILES):
        bias[at] = mask_tile(width, blocks, (2 * BLK, BLK), 1)


def key_half(steps_of, key, value, queries, stats_of, bias, dk, dv):
    for steps in steps_of:
        query = joined([queries(s, 0) for s in steps])
        grad = joined([queries(s, 1) for s in steps])
        logits2 = dot(key, query, NT)
        product2 = dot(value, grad, NT)
        probs2, change2 = [], []
        for part, step in enumerate(steps):
            log_norm, centre = stats_of(step)
            logits = logits2[:, part * BLK : (part + 1) * BLK] * SCALE2 - log_norm
            if step in B_TILES:
                logits = logits + bias[B_TILES.index(step)]
            probs = jnp.exp2(logits)
            probs2.append(probs.astype(BF))
            change = probs * (product2[:, part * BLK : (part + 1) * BLK] - centre)
            change2.append(change.astype(BF))
        probs2 = probs2[0] if len(steps) == 1 else jnp.concatenate(probs2, axis=1)
        change2 = change2[0] if len(steps) == 1 else jnp.concatenate(change2, axis=1)
        dv = dv + dot(probs2, grad, NN)
        dk = dk + dot(change2, query, NN)
    return dk, dv


def far_key_kernel(
    scal, qg, qgn, qgnn, kv, stats, near, after, part_hbm, out_hbm, bias, part, out, sem, sems_out
):
    arrived = fetch_heads(part_hbm, part, sem)
    fill_b(scal[0], bias)

    def queries(at, which, h):
        if at < SIDE:
            return qg[at, which, h]
        return qgnn[which, h] if at == 2 * SIDE else qgn[at - SIDE, which, h]

    def stats_of(at, h):
        if at < SIDE:
            return stats_rows(stats, at, h)
        return stats_rows(after, 0, h) if at == 2 * SIDE else stats_rows(near, at - SIDE, h)

    def head(h):
        arrived(h)
        for half, todo in ((0, ((0, 1), (4, 5), (6,))), (1, ((2, 3), (4, 5), (6,)))):
            j = 2 * half
            dk, dv = key_half(
                todo,
                joined([kv[j, 0, h], kv[j + 1, 0, h]]),
                joined([kv[j, 1, h], kv[j + 1, 1, h]]),
                lambda s, which: queries(j + s, which, h),
                lambda s: stats_of(j + s, h),
                bias, part[half, 0, h], part[half, 1, h],
            )
            dk = (dk * SCALE).astype(BF)
            dv = dv.astype(BF)
            out[j, 0, h] = dk[:BLK]
            out[j + 1, 0, h] = dk[BLK:]
            out[j, 1, h] = dv[:BLK]
            out[j + 1, 1, h] = dv[BLK:]
        head_copy(out, out_hbm, sems_out, h).start()

    for h in range(HC):
        head(h)
    finish_heads(out, out_hbm, sems_out)


VM = pl.BlockSpec(memory_space=pltpu.VMEM)
HBM = pl.BlockSpec(memory_space=pltpu.HBM)
PARAMS = pltpu.CompilerParams(vmem_limit_bytes=12 * 1024 * 1024)


def call(kernel, outs, scratch, scal, *args, specs=None):
    in_specs = [pl.BlockSpec(memory_space=pltpu.SMEM)] + (specs or [VM for _ in args])
    out_specs = [VM if isinstance(out, jax.ShapeDtypeStruct) else HBM for out in outs]
    return pl.pallas_call(
        kernel,
        out_shape=outs,
        in_specs=in_specs,
        out_specs=out_specs,
        scratch_shapes=scratch,
        compiler_params=PARAMS,
    )(scal, *args)


def in_hbm(value):
    return pltpu.with_memory_space_constraint(value, pltpu.HBM)


def blocks_of(arrays, blocks=SIDE):
    return jax.ShapeDtypeStruct((blocks, arrays, HC, BLK, HD), BF)


def pack(first, second):
    return pl.pallas_call(
        pack_kernel,
        out_shape=blocks_of(2),
        in_specs=[HBM, HBM],
        out_specs=VM,
        scratch_shapes=[pltpu.SemaphoreType.DMA((2 * HEADS,))],
        compiler_params=PARAMS,
    )(in_hbm(first), in_hbm(second))


def unpack(back):
    arrays = back.shape[1]
    rows = jax.ShapeDtypeStruct((BLK, HEADS * HD), BF)
    return pl.pallas_call(
        unpack_kernel,
        out_shape=[rows] * arrays,
        in_specs=[VM],
        out_specs=[HBM] * arrays,
        scratch_shapes=[pltpu.SemaphoreType.DMA((arrays * HEADS,))],
        compiler_params=PARAMS,
    )(back)


def shift(value, steps):
    count = lax.axis_size(GROUPS)
    pairs = [(at, at + steps) for at in range(count) if 0 <= at + steps < count]
    return lax.ppermute(value, GROUPS, pairs)


def swap(value):
    return lax.all_to_all(value, INSIDE, 0, 0)


def steps(queries, keys, values, grad_out, window):
    group = lax.axis_index(GROUPS)
    scal = jnp.stack([window[0], group]).astype(jnp.int32)
    packed = pack(keys, values)
    kv = swap(packed)
    packed = pack(queries, grad_out)
    raw = shift(packed, -1)
    kvp = shift(kv, 1)
    kvpp = shift(kv[SIDE - 1], 2)
    qg = swap(packed)
    qgnn = shift(qg[0], -2)
    qgn = swap(raw)
    tiles = pltpu.VMEM((5, 2 * BLK, BLK), F32)
    row_tiles = pltpu.VMEM((2, 7, 2 * BLK, BLK), F32)
    cols = pltpu.VMEM((2 * BLK, BLK), F32)
    halo = pltpu.VMEM((SIDE, 2, HC, BLK, HD), BF)
    sems = pltpu.SemaphoreType.DMA((HC,))
    part_shape = (SIDE // 2, 2, HC, 2 * BLK, HD)
    dq_late, stats_late, part = call(
        early_kernel,
        [
            blocks_of(1, 2),
            jax.ShapeDtypeStruct((16, BLK), F32),
            pltpu.HBM(part_shape, F32),
        ],
        [
            cols, tiles, tiles, row_tiles, row_tiles, halo,
            pltpu.VMEM(part_shape, F32), sems, sems,
        ],
        scal, qg, kv, in_hbm(kvp),
        specs=[VM, VM, HBM],
    )
    dq, stats, front = call(
        query_kernel,
        [
            pltpu.HBM(blocks_of(1).shape, BF),
            jax.ShapeDtypeStruct((8 * SIDE, BLK), F32),
            jax.ShapeDtypeStruct((8, BLK), F32),
        ],
        [cols, tiles, row_tiles, row_tiles, halo, pltpu.VMEM(blocks_of(1).shape, BF), sems, sems],
        scal, qg, kv, in_hbm(kvp), kvpp, dq_late, stats_late,
        specs=[VM, VM, HBM, VM, VM, VM],
    )
    near = shift(stats, -1)
    after = shift(front, -2)
    back = swap(dq)
    (query_grad,) = unpack(back)
    (dkv,) = call(
        far_key_kernel,
        [pltpu.HBM(blocks_of(2).shape, BF)],
        [
            tiles, pltpu.VMEM(part_shape, F32), pltpu.VMEM(blocks_of(2).shape, BF),
            sems, sems,
        ],
        scal, qg, qgn, qgnn, kv, stats, near, after, in_hbm(part),
        specs=[VM] * 7 + [HBM],
    )
    back = swap(dkv)
    key_grad, value_grad = unpack(back)
    return query_grad, key_grad, value_grad


def solution(mesh):
    cube = Mesh(np.asarray(mesh.devices).reshape(4, 2, 8, SIDE), GROUPS + ("x",))
    rows = P(GROUPS + ("x",), None)
    return jax.shard_map(
        steps,
        mesh=cube,
        in_specs=(rows, rows, rows, rows, P()),
        out_specs=(rows, rows, rows),
        check_vma=False,
    )
```

```python
import math

import jax
import jax.numpy as jnp
import numpy as np
from jax import lax
from jax.experimental import pallas as pl
from jax.experimental.pallas import tpu as pltpu
from jax.sharding import Mesh
from jax.sharding import PartitionSpec as P


HEADS = 16
HD = 128
BLK = 128
SIDE = 4
HC = HEADS // SIDE
SCALE = HD ** (-0.5)
SCALE2 = SCALE * math.log2(math.e)
OFF = -1e30
GROUPS = ("o", "yl", "z")
INSIDE = "x"
BF = jnp.bfloat16
F32 = jnp.float32

NT = (((1,), (1,)), ((), ()))
NN = (((1,), (0,)), ((), ()))


def dot(a, b, dims):
    return lax.dot_general(a, b, dims, preferred_element_type=F32)


def mask_tile(width, blocks, shape, query_axis):
    query = lax.broadcasted_iota(jnp.int32, shape, query_axis)
    key = lax.broadcasted_iota(jnp.int32, shape, 1 - query_axis)
    back = query - key + blocks * BLK
    return jnp.where((back >= 0) & (back < width), 0.0, OFF).astype(F32)


def pack_kernel(first, second, out, sems):
    copies = []
    for dest in range(SIDE):
        for which, ref in enumerate((first, second)):
            for h in range(HC):
                lane = (dest * HC + h) * HD
                copies.append(
                    pltpu.make_async_copy(
                        ref.at[:, lane : lane + HD], out.at[dest, which, h], sems.at[len(copies)]
                    )
                )
    for copy in copies:
        copy.start()
    for copy in copies:
        copy.wait()


def unpack_kernel(back, *rest):
    outs, sems = rest[:-1], rest[-1]
    copies = []
    for which, out in enumerate(outs):
        for source in range(SIDE):
            for h in range(HC):
                lane = (source * HC + h) * HD
                copies.append(
                    pltpu.make_async_copy(
                        back.at[source, which, h], out.at[:, lane : lane + HD], sems.at[len(copies)]
                    )
                )
    for copy in copies:
        copy.start()
    for copy in copies:
        copy.wait()


def joined(blocks):
    return blocks[0] if len(blocks) == 1 else jnp.concatenate(blocks, axis=0)


A_TILES = (5, 4, 3, 0, -1)
A_STEPS = ((6,), (4, 5), (2, 3), (0, 1))


def fill_a(width, bias):
    for at, blocks in enumerate(A_TILES):
        bias[at] = mask_tile(width, blocks, (2 * BLK, BLK), 0)


def query_half(j, h, group, qg, keys, bias, wts, prods, cols, arrived):
    shape = (2 * BLK, BLK)
    query = joined([qg[j, 0, h], qg[j + 1, 0, h]])
    grad = joined([qg[j, 1, h], qg[j + 1, 1, h]])
    norm = jnp.zeros(shape, F32)
    centre = jnp.zeros(shape, F32)
    for steps in A_STEPS:
        if j + steps[0] <= SIDE < j + steps[0] + 2:
            arrived(h)
        logits2 = dot(query, joined([keys(j + s, 0, h) for s in steps]), NT)
        product2 = dot(grad, joined([keys(j + s, 1, h) for s in steps]), NT)
        for part, step in enumerate(steps):
            at, blocks = j + step, 5 - step
            logits = logits2[:, part * BLK : (part + 1) * BLK] * SCALE2
            product = product2[:, part * BLK : (part + 1) * BLK]
            if blocks in A_TILES:
                logits = logits + bias[A_TILES.index(blocks)]
            if at <= SIDE:
                behind = group > 0 if at else group > 1
                logits = logits + jnp.where(behind, 0.0, OFF).astype(F32)
            weight = jnp.exp2(logits)
            wts[h % 2, step] = weight
            prods[h % 2, step] = product
            norm = norm + weight
            centre = centre + weight * product
    norm = jnp.sum(norm, axis=1, keepdims=True)
    inverse = 1.0 / norm
    centre = jnp.sum(centre, axis=1, keepdims=True) * inverse
    total = jnp.zeros(shape, F32)
    for steps in A_STEPS:
        change = [(wts[h % 2, s] * inverse) * (prods[h % 2, s] - centre) for s in steps]
        change = change[0] if len(steps) == 1 else jnp.concatenate(change, axis=1)
        total = total + dot(change.astype(BF), joined([keys(j + s, 0, h) for s in steps]), NN)
    lane = lax.broadcasted_iota(jnp.int32, shape, 1)
    cols[...] = jnp.where(
        lane == h, jnp.log2(norm), jnp.where(lane == HC + h, centre, cols[...])
    )
    return (total * SCALE).astype(BF)


def rows_of(cols):
    rows = jnp.transpose(cols[...])[:8]
    return rows[:, :BLK], rows[:, BLK:]


def head_copy(source, target, sems, h):
    return pltpu.make_async_copy(source.at[:, :, h], target.at[:, :, h], sems.at[h])


def finish_heads(source, target, sems):
    for h in range(HC):
        head_copy(source, target, sems, h).wait()


def fetch_heads(source, target, sems):
    def copy(h):
        return head_copy(source, target, sems, h)

    for h in range(HC):
        copy(h).start()
    return lambda h: copy(h).wait()


def early_kernel(
    scal, qg, kv, kvp_hbm, dq, stats, part_hbm, cols, bias, bias_b, wts, prods, kvp, part, sems, sems_out
):
    arrived = fetch_heads(kvp_hbm, kvp, sems)
    fill_a(scal[0], bias)
    fill_b(scal[0], bias_b)
    cols[...] = jnp.zeros_like(cols)

    def keys(at, which, h):
        return kvp[at - 1, which, h] if at <= SIDE else kv[at - SIDE - 1, which, h]

    def head(h):
        total = query_half(2, h, scal[1], qg, keys, bias, wts, prods, cols, arrived)
        dq[0, 0, h] = total[:BLK]
        dq[1, 0, h] = total[BLK:]

    for h in range(HC):
        head(h)
    stats[:8], stats[8:] = rows_of(cols)

    def leave(half, h):
        return pltpu.make_async_copy(
            part.at[half, :, h], part_hbm.at[half, :, h], sems_out.at[half, h]
        )

    def key_head(h):
        for half, steps in ((0, (2, 3)), (1, (0, 1))):
            j = 2 * half
            zero = jnp.zeros((2 * BLK, HD), F32)
            dk, dv = key_half(
                [steps],
                joined([kv[j, 0, h], kv[j + 1, 0, h]]),
                joined([kv[j, 1, h], kv[j + 1, 1, h]]),
                lambda s, which: qg[j + s, which, h],
                lambda s: stats_rows(stats, j + s - 2, h),
                bias_b, zero, zero,
            )
            part[half, 0, h] = dk
            part[half, 1, h] = dv
            leave(half, h).start()

    for h in range(HC):
        key_head(h)
    for h in range(HC):
        for half in range(2):
            leave(half, h).wait()


def query_kernel(
    scal, qg, kv, kvp_hbm, kvpp_hbm, dq_late, stats_late, dq_hbm, stats, front,
    cols, bias, wts, prods, kvp, kvpp, dq_own, sem, sems, sems_out,
):
    fetch = pltpu.make_async_copy(kvpp_hbm, kvpp, sem)
    fetch.start()
    arrived = fetch_heads(kvp_hbm, kvp, sems)
    fill_a(scal[0], bias)
    cols[...] = jnp.zeros_like(cols)
    dq_own[2:] = dq_late[...]
    stats[16:] = stats_late[...]

    def keys(at, which, h):
        if at == 0:
            return kvpp[which, h]
        return kvp[at - 1, which, h] if at <= SIDE else kv[at - SIDE - 1, which, h]

    def head(h):
        total = query_half(
            0, h, scal[1], qg, keys, bias, wts, prods, cols,
            lambda h: (arrived(h), fetch.wait() if h == 0 else None),
        )
        dq_own[0, 0, h] = total[:BLK]
        dq_own[1, 0, h] = total[BLK:]
        head_copy(dq_own, dq_hbm, sems_out, h).start()

    for h in range(HC):
        head(h)
    first, second = rows_of(cols)
    front[...] = first
    stats[:8] = first
    stats[8:16] = second
    finish_heads(dq_own, dq_hbm, sems_out)


def stats_rows(stats, block, h):
    return stats[block * 8 + h : block * 8 + h + 1], stats[block * 8 + HC + h : block * 8 + HC + h + 1]


B_TILES = (0, 1, 4, 5, 6)


def fill_b(width, bias):
    for at, blocks in enumerate(B_TILES):
        bias[at] = mask_tile(width, blocks, (2 * BLK, BLK), 1)


def key_half(steps_of, key, value, queries, stats_of, bias, dk, dv):
    for steps in steps_of:
        query = joined([queries(s, 0) for s in steps])
        grad = joined([queries(s, 1) for s in steps])
        logits2 = dot(key, query, NT)
        product2 = dot(value, grad, NT)
        probs2, change2 = [], []
        for part, step in enumerate(steps):
            log_norm, centre = stats_of(step)
            logits = logits2[:, part * BLK : (part + 1) * BLK] * SCALE2 - log_norm
            if step in B_TILES:
                logits = logits + bias[B_TILES.index(step)]
            probs = jnp.exp2(logits)
            probs2.append(probs.astype(BF))
            change = probs * (product2[:, part * BLK : (part + 1) * BLK] - centre)
            change2.append(change.astype(BF))
        probs2 = probs2[0] if len(steps) == 1 else jnp.concatenate(probs2, axis=1)
        change2 = change2[0] if len(steps) == 1 else jnp.concatenate(change2, axis=1)
        dv = dv + dot(probs2, grad, NN)
        dk = dk + dot(change2, query, NN)
    return dk, dv


def far_key_kernel(
    scal, qg, qgn, qgnn, kv, stats, near, after, part_hbm, out_hbm, bias, part, out, sem, sems_out
):
    arrived = fetch_heads(part_hbm, part, sem)
    fill_b(scal[0], bias)

    def queries(at, which, h):
        if at < SIDE:
            return qg[at, which, h]
        return qgnn[which, h] if at == 2 * SIDE else qgn[at - SIDE, which, h]

    def stats_of(at, h):
        if at < SIDE:
            return stats_rows(stats, at, h)
        return stats_rows(after, 0, h) if at == 2 * SIDE else stats_rows(near, at - SIDE, h)

    def head(h):
        for half, todo in ((0, ((0, 1), (4, 5), (6,))), (1, ((2, 3), (4, 5), (6,)))):
            j = 2 * half
            zero = jnp.zeros((2 * BLK, HD), F32)
            dk, dv = key_half(
                todo,
                joined([kv[j, 0, h], kv[j + 1, 0, h]]),
                joined([kv[j, 1, h], kv[j + 1, 1, h]]),
                lambda s, which: queries(j + s, which, h),
                lambda s: stats_of(j + s, h),
                bias, zero, zero,
            )
            if half == 0:
                arrived(h)
            dk = ((dk + part[half, 0, h]) * SCALE).astype(BF)
            dv = (dv + part[half, 1, h]).astype(BF)
            out[j, 0, h] = dk[:BLK]
            out[j + 1, 0, h] = dk[BLK:]
            out[j, 1, h] = dv[:BLK]
            out[j + 1, 1, h] = dv[BLK:]
        head_copy(out, out_hbm, sems_out, h).start()

    for h in range(HC):
        head(h)
    finish_heads(out, out_hbm, sems_out)


VM = pl.BlockSpec(memory_space=pltpu.VMEM)
HBM = pl.BlockSpec(memory_space=pltpu.HBM)
PARAMS = pltpu.CompilerParams(vmem_limit_bytes=12 * 1024 * 1024)


def call(kernel, outs, scratch, scal, *args, specs=None):
    in_specs = [pl.BlockSpec(memory_space=pltpu.SMEM)] + (specs or [VM for _ in args])
    out_specs = [VM if isinstance(out, jax.ShapeDtypeStruct) else HBM for out in outs]
    return pl.pallas_call(
        kernel,
        out_shape=outs,
        in_specs=in_specs,
        out_specs=out_specs,
        scratch_shapes=scratch,
        compiler_params=PARAMS,
    )(scal, *args)


def in_hbm(value):
    return pltpu.with_memory_space_constraint(value, pltpu.HBM)


def blocks_of(arrays, blocks=SIDE):
    return jax.ShapeDtypeStruct((blocks, arrays, HC, BLK, HD), BF)


def pack(first, second):
    return pl.pallas_call(
        pack_kernel,
        out_shape=blocks_of(2),
        in_specs=[HBM, HBM],
        out_specs=VM,
        scratch_shapes=[pltpu.SemaphoreType.DMA((2 * HEADS,))],
        compiler_params=PARAMS,
    )(in_hbm(first), in_hbm(second))


def unpack(back):
    arrays = back.shape[1]
    rows = jax.ShapeDtypeStruct((BLK, HEADS * HD), BF)
    return pl.pallas_call(
        unpack_kernel,
        out_shape=[rows] * arrays,
        in_specs=[VM],
        out_specs=[HBM] * arrays,
        scratch_shapes=[pltpu.SemaphoreType.DMA((arrays * HEADS,))],
        compiler_params=PARAMS,
    )(back)


def shift(value, steps):
    count = lax.axis_size(GROUPS)
    pairs = [(at, at + steps) for at in range(count) if 0 <= at + steps < count]
    return lax.ppermute(value, GROUPS, pairs)


def swap(value):
    return lax.all_to_all(value, INSIDE, 0, 0)


def steps(queries, keys, values, grad_out, window):
    group = lax.axis_index(GROUPS)
    scal = jnp.stack([window[0], group]).astype(jnp.int32)
    packed = pack(keys, values)
    kv = swap(packed)
    packed = pack(queries, grad_out)
    raw = shift(packed, -1)
    kvp = shift(kv, 1)
    kvpp = shift(kv[SIDE - 1], 2)
    qg = swap(packed)
    qgnn = shift(qg[0], -2)
    qgn = swap(raw)
    tiles = pltpu.VMEM((5, 2 * BLK, BLK), F32)
    row_tiles = pltpu.VMEM((2, 7, 2 * BLK, BLK), F32)
    cols = pltpu.VMEM((2 * BLK, BLK), F32)
    halo = pltpu.VMEM((SIDE, 2, HC, BLK, HD), BF)
    sems = pltpu.SemaphoreType.DMA((HC,))
    part_shape = (SIDE // 2, 2, HC, 2 * BLK, HD)
    dq_late, stats_late, part = call(
        early_kernel,
        [
            blocks_of(1, 2),
            jax.ShapeDtypeStruct((16, BLK), F32),
            pltpu.HBM(part_shape, F32),
        ],
        [
            cols, tiles, tiles, row_tiles, row_tiles, halo,
            pltpu.VMEM(part_shape, F32), sems, pltpu.SemaphoreType.DMA((2, HC)),
        ],
        scal, qg, kv, in_hbm(kvp),
        specs=[VM, VM, HBM],
    )
    dq, stats, front = call(
        query_kernel,
        [
            pltpu.HBM(blocks_of(1).shape, BF),
            jax.ShapeDtypeStruct((8 * SIDE, BLK), F32),
            jax.ShapeDtypeStruct((8, BLK), F32),
        ],
        [
            cols, tiles, row_tiles, row_tiles, halo,
            pltpu.VMEM((2, HC, BLK, HD), BF), pltpu.VMEM(blocks_of(1).shape, BF),
            pltpu.SemaphoreType.DMA(()), sems, sems,
        ],
        scal, qg, kv, in_hbm(kvp), in_hbm(kvpp), dq_late, stats_late,
        specs=[VM, VM, HBM, HBM, VM, VM],
    )
    near = shift(stats, -1)
    after = shift(front, -2)
    back = swap(dq)
    (query_grad,) = unpack(back)
    (dkv,) = call(
        far_key_kernel,
        [pltpu.HBM(blocks_of(2).shape, BF)],
        [
            tiles, pltpu.VMEM(part_shape, F32), pltpu.VMEM(blocks_of(2).shape, BF),
            sems, sems,
        ],
        scal, qg, qgn, qgnn, kv, stats, near, after, in_hbm(part),
        specs=[VM] * 7 + [HBM],
    )
    back = swap(dkv)
    key_grad, value_grad = unpack(back)
    return query_grad, key_grad, value_grad


def solution(mesh):
    cube = Mesh(np.asarray(mesh.devices).reshape(4, 2, 8, SIDE), GROUPS + ("x",))
    rows = P(GROUPS + ("x",), None)
    return jax.shard_map(
        steps,
        mesh=cube,
        in_specs=(rows, rows, rows, rows, P()),
        out_specs=(rows, rows, rows),
        check_vma=False,
    )
```
